32 devices in a mesh: ctx: 8 (over z, core), head: 4 (over y, x).
Axes of the slice: x: 2, y: 2, z: 4, core: 2. Of those that a mesh axis runs over, the one named last changes fastest.
Arguments:
- queries: bfloat16 [2048, 8192], P(('ctx', 'head')), may hold values from -100 to 100
- keys: bfloat16 [2048, 1024], P(('ctx', 'head')), may hold values from -100 to 100
- values: bfloat16 [2048, 1024], P(('ctx', 'head')), may hold values from -6 to 6
- out_grad: bfloat16 [2048, 8192], P(('ctx', 'head')), may hold values from -6 to 6
- doc_ids: int32 [2048], replicated, may hold values from 0 to 3, never falling along the last dimension, each value on 1 to 1024 neighbouring positions
Outputs:
- query_grad: float32 [2048, 8192], P(('ctx', 'head'))
- key_grad: float32 [2048, 1024], P(('ctx', 'head'))
- value_grad: float32 [2048, 1024], P(('ctx', 'head'))
The draws below stay inside these ranges and needn't reach their ends.
Inputs may be any that keep to these rules, and one draw needn't show every extreme that they name: `doc_ids`: never falling along the sequence; each document holds 1 to 1024 tokens, one exactly 1024.
All inputs are finite; a program needn't handle non-finite values.
Results may differ from the reference program's by a relative error of at most 0.004.
Values may be sent and summed in bfloat16 or wider, within the bound.
A program may use at most 64 MiB of HBM per device.

```python
import math
import jax
import jax.numpy as jnp
import numpy as np
from jax import lax

HEADS = 64
KV_HEADS = 8
HD = 128
BLK = 256
TOKENS = 2048
SPAN = 768
DOCS = 4
MOST_DOC = 1024
N_CTX = 8


def draw_pair(key):
    base = jax.random.fold_in(key, 7)
    key_q, key_k = jax.random.split(base, 2)
    key_vals = jax.random.normal(key_k, (TOKENS, KV_HEADS * HD), jnp.float32)
    query_vals = jax.random.normal(key_q, (TOKENS, HEADS * HD), jnp.float32)
    return (jnp.clip(query_vals, -100.0, 100.0), jnp.clip(key_vals, -100.0, 100.0))


def draw_queries(key, part):
    return draw_pair(key)[0].astype(jnp.bfloat16)


def draw_keys(key, part):
    return draw_pair(key)[1].astype(jnp.bfloat16)


def level_of(stream_key, extent, shards, least, high):
    loudness, own = 1.0, jax.random.fold_in(stream_key, 6)
    for axis_at, shards_of in shards:
        steps = jnp.exp(jax.random.uniform(jax.random.fold_in(own, axis_at), (shards_of,), jnp.float32, least / len(shards), high / len(shards)))
        loudness = loudness * jnp.repeat(steps, extent[axis_at] // shards_of).reshape([-1 if axis == axis_at else 1 for axis in range(len(extent))])
    return loudness


def profile(count, total, limit, slope):
    portions = [(1 << 20) // math.isqrt(rank ** slope) + 1 for rank in range(2, count + 1)]
    spare, given = total - limit - (count - 1), [1] * (count - 1)
    while spare > 0:
        free = [i for i in range(count - 1) if given[i] < limit]
        mass, budget = sum([portions[i] for i in free]), spare
        for i in free:
            more = min(limit - given[i], max(1, budget * portions[i] // mass), spare)
            given[i] = given[i] + more
            spare = spare - more
    return np.array([limit] + given)


def uneven_parts(stream_key, count, total, most, lean):
    if count == 2:
        one = jax.random.randint(stream_key, (), max(1, total - most), min(most, total - 1) + 1)
        return jnp.stack([one, total - one])
    tallies = jnp.asarray(profile(count, total, most, lean), jnp.int32)
    couples = (count - 1) // 2
    donor, sink = tallies[1:1 + 2 * couples:2], tallies[2:2 + 2 * couples:2]
    room = jnp.minimum(donor - 1, most - sink)
    passed = jax.random.randint(jax.random.fold_in(stream_key, 1), (couples,), 0, 1 << 20) % (room + 1)
    tallies = tallies.at[1:1 + 2 * couples:2].set(donor - passed).at[2:2 + 2 * couples:2].set(sink + passed)
    return tallies[jax.random.permutation(jax.random.fold_in(stream_key, 2), count)]


def bell_draw(own_key, extent, width, most, shards=(), kind=jnp.bfloat16):
    factor_of = level_of(own_key, extent, shards, -0.22, 0.18) if shards else 1.0
    entries = jax.random.normal(own_key, extent, jnp.float32) * width * factor_of
    return jnp.minimum(jnp.maximum(entries, -most), most).astype(kind)


def setup_inputs(seed: int = 0) -> dict:
    streams_of = jax.random.split(jax.random.key(seed), 6)
    queries = draw_queries(jax.random.fold_in(streams_of[5], 71), 0)
    keys = draw_keys(jax.random.fold_in(streams_of[5], 71), 0)
    values = bell_draw(streams_of[2], (TOKENS, KV_HEADS * HD), 1.0, 6.0, ((0, 32),))
    out_grad = bell_draw(streams_of[3], (TOKENS, HEADS * HD), 1.0, 6.0, ((0, 32),))
    doc_ids = jnp.searchsorted(jnp.cumsum(uneven_parts(streams_of[4], DOCS, TOKENS, MOST_DOC, 2)), jnp.arange(TOKENS), side="right").astype(jnp.int32)
    return {"queries": queries, "keys": keys, "values": values, "out_grad": out_grad, "doc_ids": doc_ids}


def reference(queries, keys, values, out_grad, doc_ids):
    group_size = HEADS // KV_HEADS
    score_scale = 1.0 / (HD ** 0.5)
    margin = 3 * BLK
    pad_keys = jnp.concatenate([jnp.zeros((margin, KV_HEADS * HD), keys.dtype), keys], 0)
    pad_values = jnp.concatenate([jnp.zeros((margin, KV_HEADS * HD), values.dtype), values], 0)
    pad_docs = jnp.concatenate([jnp.full((margin,), -1, jnp.int32), doc_ids.astype(jnp.int32)], 0)
    zero_acc = jnp.zeros((margin + TOKENS, KV_HEADS, HD), jnp.float32)

    def one_block(carry, block):
        key_acc, value_acc = carry
        first_row = (block * BLK).astype(jnp.int32)
        key_win = lax.dynamic_slice_in_dim(pad_keys, first_row, 4 * BLK, 0).reshape(4 * BLK, KV_HEADS, HD).astype(jnp.float32)
        value_win = lax.dynamic_slice_in_dim(pad_values, first_row, 4 * BLK, 0).reshape(4 * BLK, KV_HEADS, HD).astype(jnp.float32)
        query_blk = lax.dynamic_slice_in_dim(queries, first_row, BLK, 0).reshape(BLK, KV_HEADS, group_size, HD).astype(jnp.float32)
        grad_blk = lax.dynamic_slice_in_dim(out_grad, first_row, BLK, 0).reshape(BLK, KV_HEADS, group_size, HD).astype(jnp.float32)
        query_pos = first_row + jnp.arange(BLK, dtype=jnp.int32)
        key_pos = first_row - margin + jnp.arange(4 * BLK, dtype=jnp.int32)
        query_doc = lax.dynamic_slice_in_dim(doc_ids.astype(jnp.int32), first_row, BLK, 0)
        key_doc = lax.dynamic_slice_in_dim(pad_docs, first_row, 4 * BLK, 0)
        allowed = (key_pos[None, :] <= query_pos[:, None]) & (key_pos[None, :] > query_pos[:, None] - SPAN)
        allowed = allowed & (key_pos[None, :] >= 0) & (query_doc[:, None] == key_doc[None, :])
        scores = jnp.einsum('ikgd,jkd->kgij', query_blk, key_win) * score_scale
        scores = jnp.where(allowed[None, None], scores, -jnp.inf)
        row_max = jnp.max(scores, -1, keepdims=True)
        expo = jnp.exp(scores - row_max)
        weights = expo / jnp.sum(expo, -1, keepdims=True)
        weight_bf = lax.optimization_barrier(weights.astype(jnp.bfloat16)).astype(jnp.float32)
        attended = jnp.einsum('kgij,jkd->ikgd', weight_bf, value_win)
        delta_sum = jnp.transpose(jnp.sum(grad_blk * attended, -1), (1, 2, 0))
        value_part = jnp.einsum('kgij,ikgd->jkd', weight_bf, grad_blk)
        prob_grad = jnp.einsum('ikgd,jkd->kgij', grad_blk, value_win)
        score_grad = lax.optimization_barrier((weights * (prob_grad - delta_sum[..., None])).astype(jnp.bfloat16)).astype(jnp.float32)
        query_full = jnp.einsum('kgij,jkd->ikgd', score_grad, key_win) * score_scale
        key_part = jnp.einsum('kgij,ikgd->jkd', score_grad, query_blk) * score_scale
        zero = jnp.zeros((), jnp.int32)
        key_old = lax.dynamic_slice(key_acc, (first_row, zero, zero), (4 * BLK, KV_HEADS, HD))
        key_acc = lax.dynamic_update_slice(key_acc, key_old + key_part, (first_row, zero, zero))
        value_old = lax.dynamic_slice(value_acc, (first_row, zero, zero), (4 * BLK, KV_HEADS, HD))
        value_acc = lax.dynamic_update_slice(value_acc, value_old + value_part, (first_row, zero, zero))
        return (key_acc, value_acc), query_full.reshape(BLK, HEADS * HD)

    (key_acc, value_acc), query_rows = lax.scan(one_block, (zero_acc, zero_acc), jnp.arange(N_CTX, dtype=jnp.int32))
    query_full = query_rows.reshape(TOKENS, HEADS * HD)
    key_full = key_acc[margin:].reshape(TOKENS, KV_HEADS * HD)
    value_full = value_acc[margin:].reshape(TOKENS, KV_HEADS * HD)
    return (query_full, key_full, value_full)
```

```python
import functools
import math
import jax
import jax.numpy as jnp
from jax import lax
from jax.experimental import pallas as pl
from jax.experimental.pallas import tpu as pltpu
from jax.sharding import PartitionSpec as P

HD = 128
BACK = 3
CHUNK = 2
MESH = pl.DeviceIdType.MESH
NT = (((1,), (1,)), ((), ()))


def kernel(
    n_ctx, n_head, group,
    q_ref, k_ref, v_ref, g_ref, doc_ref,
    dq_out, dk_out, dv_out,
    q_buf, g_buf, dq_buf, kv_buf, kt_buf, acc, bias, part_out, part_in, own_part, tot,
    own_sem, kv_send, kv_recv, ctx_send, ctx_recv, in_send, in_recv,
    dq_send, dq_recv, part_send, part_recv, tot_send, tot_recv,
):
    c = lax.axis_index("ctx")
    h = lax.axis_index("head")
    rows = q_ref.shape[0]
    blk = rows * n_head
    kv_n = kv_buf.shape[0]
    n_chunk, _, width = q_buf.shape
    per_kv = n_chunk // kv_n
    cols = n_chunk * width
    scale = 1.0 / HD**0.5
    spread = range(1, BACK + 1)

    def peer(p):
        other, bit = 0, 1
        while bit < n_head:
            other = other + ((h // bit) % 2 + (p // bit) % 2) % 2 * bit
            bit *= 2
        return other

    barrier = pltpu.get_barrier_semaphore()
    for p in range(1, n_head):
        pl.semaphore_signal(barrier, inc=1, device_id=(c, peer(p)), device_id_type=MESH)
    for s in spread:
        for to in ((c + s) % n_ctx, (c - s + n_ctx) % n_ctx):
            pl.semaphore_signal(barrier, inc=1, device_id=(to, h), device_id_type=MESH)
    pl.semaphore_wait(barrier, n_head - 1 + 2 * BACK)

    def at(n, size):
        return pl.ds(pl.multiple_of(n * size, size), size)

    def kv_copy(kv, t, p):
        to = peer(p)
        ref = (k_ref, v_ref)[t]
        return pltpu.make_async_remote_copy(
            src_ref=ref.at[:, at(to * kv_n + kv, HD)],
            dst_ref=kv_buf.at[kv, BACK, t, at(h, rows)],
            send_sem=kv_send.at[kv, t, p - 1],
            recv_sem=kv_recv.at[kv, t, p - 1],
            device_id=(c, to), device_id_type=MESH,
        )

    def kv_own(kv, t):
        ref = (k_ref, v_ref)[t]
        return pltpu.make_async_copy(
            ref.at[:, at(h * kv_n + kv, HD)], kv_buf.at[kv, BACK, t, at(h, rows)],
            own_sem.at[kv, t],
        )

    def in_copy(ch, t, p):
        to = peer(p)
        return pltpu.make_async_remote_copy(
            src_ref=(q_ref, g_ref)[t].at[:, at(to * n_chunk + ch, width)],
            dst_ref=(q_buf, g_buf)[t].at[ch, at(h, rows)],
            send_sem=in_send.at[ch, t, p - 1],
            recv_sem=in_recv.at[ch, t, p - 1],
            device_id=(c, to), device_id_type=MESH,
        )

    def in_own(ch, t):
        return pltpu.make_async_copy(
            (q_ref, g_ref)[t].at[:, at(h * n_chunk + ch, width)],
            (q_buf, g_buf)[t].at[ch, at(h, rows)],
            in_recv.at[ch, t, n_head - 1],
        )

    def ctx_copy(kv, s):
        return pltpu.make_async_remote_copy(
            src_ref=kv_buf.at[kv, BACK], dst_ref=kv_buf.at[kv, BACK - s],
            send_sem=ctx_send.at[kv, s - 1], recv_sem=ctx_recv.at[kv, s - 1],
            device_id=((c + s) % n_ctx, h), device_id_type=MESH,
        )

    def dq_copy(ch, p):
        to = peer(p)
        return pltpu.make_async_remote_copy(
            src_ref=dq_buf.at[ch, at(to, rows)],
            dst_ref=dq_out.at[:, at(h * n_chunk + ch, width)],
            send_sem=dq_send.at[ch, p - 1], recv_sem=dq_recv.at[ch, p - 1],
            device_id=(c, to), device_id_type=MESH,
        )

    def dq_own(ch):
        return pltpu.make_async_copy(
            dq_buf.at[ch, at(h, rows)], dq_out.at[:, at(h * n_chunk + ch, width)],
            dq_send.at[ch, n_head - 1],
        )

    def part_copy(kv, s):
        return pltpu.make_async_remote_copy(
            src_ref=part_out.at[kv, s - 1], dst_ref=part_in.at[kv, s - 1],
            send_sem=part_send.at[kv, s - 1], recv_sem=part_recv.at[kv, s - 1],
            device_id=((c - s + n_ctx) % n_ctx, h), device_id_type=MESH,
        )

    def tot_copy(kv, t, p):
        to = peer(p)
        return pltpu.make_async_remote_copy(
            src_ref=tot.at[kv, t, at(to, rows)],
            dst_ref=(dk_out, dv_out)[t].at[:, at(h * kv_n + kv, HD)],
            send_sem=tot_send.at[kv, t, p - 1], recv_sem=tot_recv.at[kv, t, p - 1],
            device_id=(c, to), device_id_type=MESH,
        )

    def tot_own(kv, t):
        return pltpu.make_async_copy(
            tot.at[kv, t, at(h, rows)], (dk_out, dv_out)[t].at[:, at(h * kv_n + kv, HD)],
            tot_send.at[kv, t, n_head - 1],
        )

    others = range(1, n_head)
    for kv in range(kv_n):
        for t in range(2):
            for p in others:
                kv_copy(kv, t, p).start()
            kv_own(kv, t).start()

    @pl.loop(0, n_chunk)
    def _(ch):
        for t in range(2):
            for p in others:
                in_copy(ch, t, p).start()
            in_own(ch, t).start()

    for kv in range(kv_n):
        for t in range(2):
            kv_own(kv, t).wait()
            for p in others:
                kv_copy(kv, t, p).wait_recv()
        for s in spread:
            @pl.when(c + s < n_ctx)
            def _():
                ctx_copy(kv, s).start()

            @pl.when(c < s)
            def _():
                kv_buf[kv, BACK - s] = jnp.zeros(kv_buf.shape[2:], kv_buf.dtype)

    tile = HD
    query_doc = doc_ref[:, pl.ds(pl.multiple_of(c * blk, blk), blk)].astype(jnp.float32)
    for part in range(4 * blk // tile):
        key_blk = jnp.maximum(c - BACK + part * tile // blk, 0)
        start = pl.multiple_of(key_blk * blk + part * tile % blk, tile)
        key_row = doc_ref[:, pl.ds(start, tile)].astype(jnp.float32)
        key_doc = jnp.transpose(jnp.broadcast_to(key_row, (tile, tile)))
        key_doc = jnp.concatenate([key_doc] * (blk // tile), axis=1)
        j = lax.broadcasted_iota(jnp.int32, (tile, blk), 0) + part * tile
        i = lax.broadcasted_iota(jnp.int32, (tile, blk), 1)
        ok = (j > i) & (j <= i + BACK * blk) & (j + (c - BACK) * blk >= 0)
        ok = ok & (key_doc == query_doc)
        bias[pl.ds(part * tile, tile)] = jnp.where(ok, 0.0, -1e30)

    for kv in range(kv_n):
        for s in spread:
            @pl.when(c >= s)
            def _():
                ctx_copy(kv, s).wait_recv()

        keys = kv_buf[kv, :, 0].reshape(4 * blk, HD)
        kt_buf[...] = jnp.transpose(keys.astype(jnp.float32)).astype(jnp.bfloat16)
        acc[...] = jnp.zeros(acc.shape, acc.dtype)

        @pl.loop(0, per_kv)
        def _(step):
            ch = kv * per_kv + step
            for t in range(2):
                in_own(ch, t).wait()
                for p in others:
                    in_copy(ch, t, p).wait_recv()
            for a in range(width // HD):
                lanes = pl.ds(a * HD, HD)
                q = q_buf[ch, :, lanes]
                g = g_buf[ch, :, lanes]
                key_win = kv_buf[kv, :, 0].reshape(4 * blk, HD)
                val_win = kv_buf[kv, :, 1].reshape(4 * blk, HD)
                s_t = lax.dot_general(key_win, q, NT, preferred_element_type=jnp.float32)
                s_t = s_t + bias[...]
                top = jnp.max(s_t, axis=0, keepdims=True)
                e_t = jnp.exp2((s_t - top) * (scale * math.log2(math.e)))
                w_t = e_t * (1.0 / jnp.sum(e_t, axis=0, keepdims=True))
                w_bf = w_t.astype(jnp.bfloat16)
                p_t = lax.dot_general(val_win, g, NT, preferred_element_type=jnp.float32)
                delta = jnp.sum(w_bf.astype(jnp.float32) * p_t, axis=0, keepdims=True)
                d_t = (w_t * (p_t - delta)).astype(jnp.bfloat16)
                dv = jnp.dot(w_bf, g, preferred_element_type=jnp.float32)
                dk = jnp.dot(d_t, q, preferred_element_type=jnp.float32)
                acc[:, 0] += dk.reshape(4, blk, HD)
                acc[:, 1] += dv.reshape(4, blk, HD)
                dq_t = jnp.dot(kt_buf[...], d_t, preferred_element_type=jnp.float32)
                dq_buf[ch, :, lanes] = jnp.transpose(dq_t * scale).astype(jnp.bfloat16)
            for p in others:
                dq_copy(ch, p).start()
            dq_own(ch).start()

        for s in spread:
            part_out[kv, s - 1, 0] = (acc[BACK - s, 0] * scale).astype(jnp.bfloat16)
            part_out[kv, s - 1, 1] = acc[BACK - s, 1].astype(jnp.bfloat16)

            @pl.when(c >= s)
            def _():
                part_copy(kv, s).start()
        own_part[kv, 0] = acc[BACK, 0] * scale
        own_part[kv, 1] = acc[BACK, 1]

    for kv in range(kv_n):
        for s in spread:
            @pl.when(c + s < n_ctx)
            def _():
                part_copy(kv, s).wait_recv()
                own_part[kv] += part_in[kv, s - 1].astype(jnp.float32)

        tot[kv] = own_part[kv].astype(jnp.bfloat16)
        for t in range(2):
            for p in others:
                tot_copy(kv, t, p).start()
            tot_own(kv, t).start()

    @pl.loop(0, n_chunk)
    def _(ch):
        for t in range(2):
            for p in others:
                in_copy(ch, t, p).wait_send()
        for p in others:
            dq_copy(ch, p).wait()
        dq_own(ch).wait()

    for kv in range(kv_n):
        for t in range(2):
            for p in others:
                kv_copy(kv, t, p).wait_send()
                tot_copy(kv, t, p).wait()
            tot_own(kv, t).wait()
        for s in spread:
            @pl.when(c + s < n_ctx)
            def _():
                ctx_copy(kv, s).wait_send()

            @pl.when(c >= s)
            def _():
                part_copy(kv, s).wait_send()


def body(queries, keys, values, out_grad, doc_ids):
    n_ctx, n_head = lax.axis_size("ctx"), lax.axis_size("head")
    rows, q_cols = queries.shape
    kv_cols = keys.shape[1]
    blk = rows * n_head
    kv_n = kv_cols // HD // n_head
    group = q_cols // kv_cols
    chunk = math.gcd(CHUNK, group)
    width = chunk * HD
    n_chunk = kv_n * group // chunk
    win = BACK + 1
    bf, f32, dma = jnp.bfloat16, jnp.float32, pltpu.SemaphoreType.DMA
    far = pl.BlockSpec(memory_space=pl.ANY)
    near = pl.BlockSpec(memory_space=pltpu.VMEM)
    dq, dk, dv = pl.pallas_call(
        functools.partial(kernel, n_ctx, n_head, group),
        out_shape=(
            jax.ShapeDtypeStruct((rows, q_cols), bf),
            jax.ShapeDtypeStruct((rows, kv_cols), bf),
            jax.ShapeDtypeStruct((rows, kv_cols), bf),
        ),
        in_specs=[far, far, far, far, near],
        out_specs=(far, far, far),
        scratch_shapes=[
            pltpu.VMEM((n_chunk, blk, width), bf),
            pltpu.VMEM((n_chunk, blk, width), bf),
            pltpu.VMEM((n_chunk, blk, width), bf),
            pltpu.VMEM((kv_n, win, 2, blk, HD), bf),
            pltpu.VMEM((HD, win * blk), bf),
            pltpu.VMEM((win, 2, blk, HD), f32),
            pltpu.VMEM((win * blk, blk), f32),
            pltpu.VMEM((kv_n, BACK, 2, blk, HD), bf),
            pltpu.VMEM((kv_n, BACK, 2, blk, HD), bf),
            pltpu.VMEM((kv_n, 2, blk, HD), f32),
            pltpu.VMEM((kv_n, 2, blk, HD), bf),
            dma((kv_n, 2)),
            dma((kv_n, 2, n_head)),
            dma((kv_n, 2, n_head)),
            dma((kv_n, BACK)),
            dma((kv_n, BACK)),
            dma((n_chunk, 2, n_head)),
            dma((n_chunk, 2, n_head)),
            dma((n_chunk, n_head)),
            dma((n_chunk, n_head)),
            dma((kv_n, BACK)),
            dma((kv_n, BACK)),
            dma((kv_n, 2, n_head)),
            dma((kv_n, 2, n_head)),
        ],
        compiler_params=pltpu.CompilerParams(
            collective_id=0, has_side_effects=True, vmem_limit_bytes=56 * 2**20
        ),
    )(queries, keys, values, out_grad, doc_ids.reshape(1, -1))
    return dq.astype(f32), dk.astype(f32), dv.astype(f32)


def solution(mesh):
    split = P(("ctx", "head"), None)
    return jax.shard_map(
        body,
        mesh=mesh,
        in_specs=(split, split, split, split, P()),
        out_specs=(split, split, split),
        check_vma=False,
    )
```

```python
import functools
import math
import jax
import jax.numpy as jnp
from jax import lax
from jax.experimental import pallas as pl
from jax.experimental.pallas import tpu as pltpu
from jax.sharding import PartitionSpec as P

HD = 128
SPLIT = 2
WINDOW = 3
CHUNK = 4
STACK = 2
MESH = pl.DeviceIdType.MESH
NT = (((1,), (1,)), ((), ()))


def kernel(
    n_ctx, n_head, group,
    q_ref, k_ref, v_ref, g_ref, doc_ref,
    dq_out, dk_out, dv_out,
    q_buf, g_buf, dq_buf, kv_buf, kt_buf, acc, bias, part_out, part_in, own_part, tot,
    own_sem, kv_send, kv_recv, ctx_send, ctx_recv, in_send, in_recv,
    dq_send, dq_recv, part_send, part_recv, tot_send, tot_recv,
):
    c = lax.axis_index("ctx")
    h = lax.axis_index("head")
    high = n_head // SPLIT
    low = h % SPLIT
    here = c * high + h // SPLIT
    n_blk = n_ctx * high
    back = WINDOW * high
    rows = q_ref.shape[0]
    blk = rows * SPLIT
    win = (back + 1) * blk
    kv_n = kv_buf.shape[0]
    n_chunk, _, width = q_buf.shape
    per_kv = n_chunk // kv_n
    cols = n_chunk * width
    scale = 1.0 / HD**0.5
    spread = range(1, back + 1)

    def peer(p):
        return (low + p) % SPLIT

    def mate(p):
        return (c, h - low + peer(p))

    def device(b):
        return (b // high, b % high * SPLIT + low)

    barrier = pltpu.get_barrier_semaphore()
    for p in range(1, SPLIT):
        pl.semaphore_signal(barrier, inc=1, device_id=mate(p), device_id_type=MESH)
    for s in spread:
        for b in ((here + s) % n_blk, (here - s + n_blk) % n_blk):
            pl.semaphore_signal(barrier, inc=1, device_id=device(b), device_id_type=MESH)
    pl.semaphore_wait(barrier, SPLIT - 1 + 2 * back)

    def at(n, size):
        return pl.ds(pl.multiple_of(n * size, size), size)

    def kv_copy(kv, t, p):
        to = peer(p)
        ref = (k_ref, v_ref)[t]
        return pltpu.make_async_remote_copy(
            src_ref=ref.at[:, at(to * kv_n + kv, HD)],
            dst_ref=kv_buf.at[kv, back, t, at(low, rows)],
            send_sem=kv_send.at[kv, t, p - 1],
            recv_sem=kv_recv.at[kv, t, p - 1],
            device_id=mate(p), device_id_type=MESH,
        )

    def kv_own(kv, t):
        ref = (k_ref, v_ref)[t]
        return pltpu.make_async_copy(
            ref.at[:, at(low * kv_n + kv, HD)], kv_buf.at[kv, back, t, at(low, rows)],
            own_sem.at[kv, t],
        )

    def in_copy(ch, t, p):
        to = peer(p)
        return pltpu.make_async_remote_copy(
            src_ref=(q_ref, g_ref)[t].at[:, at(to * n_chunk + ch, width)],
            dst_ref=(q_buf, g_buf)[t].at[ch, at(low, rows)],
            send_sem=in_send.at[ch, t, p - 1],
            recv_sem=in_recv.at[ch, t, p - 1],
            device_id=mate(p), device_id_type=MESH,
        )

    def in_own(ch, t):
        return pltpu.make_async_copy(
            (q_ref, g_ref)[t].at[:, at(low * n_chunk + ch, width)],
            (q_buf, g_buf)[t].at[ch, at(low, rows)],
            in_recv.at[ch, t, SPLIT - 1],
        )

    def ctx_copy(kv, s):
        return pltpu.make_async_remote_copy(
            src_ref=kv_buf.at[kv, back], dst_ref=kv_buf.at[kv, back - s],
            send_sem=ctx_send.at[kv, s - 1], recv_sem=ctx_recv.at[kv, s - 1],
            device_id=device((here + s) % n_blk), device_id_type=MESH,
        )

    def dq_copy(ch, p):
        to = peer(p)
        return pltpu.make_async_remote_copy(
            src_ref=dq_buf.at[ch, at(to, rows)],
            dst_ref=dq_out.at[:, at(low * n_chunk + ch, width)],
            send_sem=dq_send.at[ch, p - 1], recv_sem=dq_recv.at[ch, p - 1],
            device_id=mate(p), device_id_type=MESH,
        )

    def dq_own(ch):
        return pltpu.make_async_copy(
            dq_buf.at[ch, at(low, rows)], dq_out.at[:, at(low * n_chunk + ch, width)],
            dq_send.at[ch, SPLIT - 1],
        )

    def part_copy(kv, s):
        return pltpu.make_async_remote_copy(
            src_ref=part_out.at[kv, s - 1], dst_ref=part_in.at[kv, s - 1],
            send_sem=part_send.at[kv, s - 1], recv_sem=part_recv.at[kv, s - 1],
            device_id=device((here - s + n_blk) % n_blk), device_id_type=MESH,
        )

    def tot_copy(kv, t, p):
        to = peer(p)
        return pltpu.make_async_remote_copy(
            src_ref=tot.at[kv, t, at(to, rows)],
            dst_ref=(dk_out, dv_out)[t].at[:, at(low * kv_n + kv, HD)],
            send_sem=tot_send.at[kv, t, p - 1], recv_sem=tot_recv.at[kv, t, p - 1],
            device_id=mate(p), device_id_type=MESH,
        )

    def tot_own(kv, t):
        return pltpu.make_async_copy(
            tot.at[kv, t, at(low, rows)], (dk_out, dv_out)[t].at[:, at(low * kv_n + kv, HD)],
            tot_send.at[kv, t, SPLIT - 1],
        )

    others = range(1, SPLIT)
    for kv in range(kv_n):
        for t in range(2):
            for p in others:
                kv_copy(kv, t, p).start()
            kv_own(kv, t).start()

    @pl.loop(0, n_chunk)
    def _(ch):
        for t in range(2):
            for p in others:
                in_copy(ch, t, p).start()
            in_own(ch, t).start()

    for kv in range(kv_n):
        for t in range(2):
            kv_own(kv, t).wait()
            for p in others:
                kv_copy(kv, t, p).wait_recv()
        for s in spread:
            @pl.when(here + s < n_blk)
            def _():
                ctx_copy(kv, s).start()

            @pl.when(here < s)
            def _():
                kv_buf[kv, back - s] = jnp.zeros(kv_buf.shape[2:], kv_buf.dtype)

    query_doc = doc_ref[pl.ds(here, 1), :].astype(jnp.float32)
    for part in range(back + 1):
        key_row = doc_ref[pl.ds(jnp.maximum(here - back + part, 0), 1), :].astype(jnp.float32)
        key_doc = jnp.transpose(jnp.broadcast_to(key_row, (blk, blk)))
        j = lax.broadcasted_iota(jnp.int32, (blk, blk), 0) + part * blk
        i = lax.broadcasted_iota(jnp.int32, (blk, blk), 1)
        ok = (j > i) & (j <= i + back * blk) & (here - back + part >= 0)
        ok = ok & (key_doc == query_doc)
        bias[pl.ds(part * blk, blk)] = jnp.where(ok, 0.0, -1e30)

    def finish(kv):
        for s in spread:
            @pl.when(here + s < n_blk)
            def _():
                part_copy(kv, s).wait_recv()
                own_part[kv] += part_in[kv, s - 1].astype(jnp.float32)

        tot[kv] = own_part[kv].astype(jnp.bfloat16)
        for t in range(2):
            for p in others:
                tot_copy(kv, t, p).start()
            tot_own(kv, t).start()

    for kv in range(kv_n):
        for s in spread:
            @pl.when(here >= s)
            def _():
                ctx_copy(kv, s).wait_recv()

        keys = kv_buf[kv, :, 0].reshape(win, HD)
        kt_buf[...] = jnp.transpose(keys.astype(jnp.float32)).astype(jnp.bfloat16)
        acc[...] = jnp.zeros(acc.shape, acc.dtype)

        @pl.loop(0, per_kv)
        def _(step):
            ch = kv * per_kv + step
            for t in range(2):
                in_own(ch, t).wait()
                for p in others:
                    in_copy(ch, t, p).wait_recv()
            for a in range(0, width // HD, STACK):
                lanes = [pl.ds((a + k) * HD, HD) for k in range(STACK)]
                q = jnp.concatenate([q_buf[ch, :, at_a] for at_a in lanes], axis=0)
                g = jnp.concatenate([g_buf[ch, :, at_a] for at_a in lanes], axis=0)
                key_win = kv_buf[kv, :, 0].reshape(win, HD)
                val_win = kv_buf[kv, :, 1].reshape(win, HD)
                s_t = lax.dot_general(key_win, q, NT, preferred_element_type=jnp.float32)
                s_t = s_t + jnp.concatenate([bias[...]] * STACK, axis=1)
                top = jnp.max(s_t, axis=0, keepdims=True)
                e_t = jnp.exp2((s_t - top) * (scale * math.log2(math.e)))
                w_t = e_t * (1.0 / jnp.sum(e_t, axis=0, keepdims=True))
                w_bf = w_t.astype(jnp.bfloat16)
                p_t = lax.dot_general(val_win, g, NT, preferred_element_type=jnp.float32)
                delta = jnp.sum(w_bf.astype(jnp.float32) * p_t, axis=0, keepdims=True)
                d_t = (w_t * (p_t - delta)).astype(jnp.bfloat16)
                dv = jnp.dot(w_bf, g, preferred_element_type=jnp.float32)
                dk = jnp.dot(d_t, q, preferred_element_type=jnp.float32)
                acc[:, 0] += dk.reshape(back + 1, blk, HD)
                acc[:, 1] += dv.reshape(back + 1, blk, HD)
                dq_t = jnp.dot(kt_buf[...], d_t, preferred_element_type=jnp.float32)
                dq = jnp.transpose(dq_t * scale).astype(jnp.bfloat16)
                for k, at_a in enumerate(lanes):
                    dq_buf[ch, :, at_a] = dq[k * blk : (k + 1) * blk]
            for p in others:
                dq_copy(ch, p).start()
            dq_own(ch).start()

        for s in spread:
            part_out[kv, s - 1, 0] = (acc[back - s, 0] * scale).astype(jnp.bfloat16)
            part_out[kv, s - 1, 1] = acc[back - s, 1].astype(jnp.bfloat16)

            @pl.when(here >= s)
            def _():
                part_copy(kv, s).start()
        own_part[kv, 0] = acc[back, 0] * scale
        own_part[kv, 1] = acc[back, 1]
        if kv:
            finish(kv - 1)

    finish(kv_n - 1)

    @pl.loop(0, n_chunk)
    def _(ch):
        for t in range(2):
            for p in others:
                in_copy(ch, t, p).wait_send()
        for p in others:
            dq_copy(ch, p).wait()
        dq_own(ch).wait()

    for kv in range(kv_n):
        for t in range(2):
            for p in others:
                kv_copy(kv, t, p).wait_send()
                tot_copy(kv, t, p).wait()
            tot_own(kv, t).wait()
        for s in spread:
            @pl.when(here + s < n_blk)
            def _():
                ctx_copy(kv, s).wait_send()

            @pl.when(here >= s)
            def _():
                part_copy(kv, s).wait_send()


def body(queries, keys, values, out_grad, doc_ids):
    n_ctx, n_head = lax.axis_size("ctx"), lax.axis_size("head")
    rows, q_cols = queries.shape
    kv_cols = keys.shape[1]
    blk = rows * SPLIT
    kv_n = kv_cols // HD // SPLIT
    back = WINDOW * (n_head // SPLIT)
    group = q_cols // kv_cols
    chunk = math.gcd(CHUNK, group)
    width = chunk * HD
    n_chunk = kv_n * group // chunk
    win = back + 1
    bf, f32, dma = jnp.bfloat16, jnp.float32, pltpu.SemaphoreType.DMA
    far = pl.BlockSpec(memory_space=pl.ANY)
    near = pl.BlockSpec(memory_space=pltpu.VMEM)
    dq, dk, dv = pl.pallas_call(
        functools.partial(kernel, n_ctx, n_head, group),
        out_shape=(
            jax.ShapeDtypeStruct((rows, q_cols), bf),
            jax.ShapeDtypeStruct((rows, kv_cols), bf),
            jax.ShapeDtypeStruct((rows, kv_cols), bf),
        ),
        in_specs=[far, far, far, far, near],
        out_specs=(far, far, far),
        scratch_shapes=[
            pltpu.VMEM((n_chunk, blk, width), bf),
            pltpu.VMEM((n_chunk, blk, width), bf),
            pltpu.VMEM((n_chunk, blk, width), bf),
            pltpu.VMEM((kv_n, win, 2, blk, HD), bf),
            pltpu.VMEM((HD, win * blk), bf),
            pltpu.VMEM((win, 2, blk, HD), f32),
            pltpu.VMEM((win * blk, blk), f32),
            pltpu.VMEM((kv_n, back, 2, blk, HD), bf),
            pltpu.VMEM((kv_n, back, 2, blk, HD), bf),
            pltpu.VMEM((kv_n, 2, blk, HD), f32),
            pltpu.VMEM((kv_n, 2, blk, HD), bf),
            dma((kv_n, 2)),
            dma((kv_n, 2, SPLIT)),
            dma((kv_n, 2, SPLIT)),
            dma((kv_n, back)),
            dma((kv_n, back)),
            dma((n_chunk, 2, SPLIT)),
            dma((n_chunk, 2, SPLIT)),
            dma((n_chunk, SPLIT)),
            dma((n_chunk, SPLIT)),
            dma((kv_n, back)),
            dma((kv_n, back)),
            dma((kv_n, 2, SPLIT)),
            dma((kv_n, 2, SPLIT)),
        ],
        compiler_params=pltpu.CompilerParams(
            collective_id=0, has_side_effects=True, vmem_limit_bytes=56 * 2**20
        ),
    )(queries, keys, values, out_grad, doc_ids.reshape(-1, blk))
    return dq.astype(f32), dk.astype(f32), dv.astype(f32)


def solution(mesh):
    split = P(("ctx", "head"), None)
    return jax.shard_map(
        body,
        mesh=mesh,
        in_specs=(split, split, split, split, P()),
        out_specs=(split, split, split),
        check_vma=False,
    )
```
